32 devices in a mesh: grp: 4 (over x, core), row: 4 (over z), col: 2 (over y).
Axes of the slice: x: 2, y: 2, z: 4, core: 2. Of those that a mesh axis runs over, the one named last changes fastest.
Arguments:
- cover: float32 [4, 12288, 4096], P('grp', 'row', 'col'), may hold values from -4 to 12, as said below
- prior: float32 [4096, 4096], P(('grp', 'row'), 'col'), may hold values from -0.5 to 2, as said below
Outputs:
- cover_out: float32 [4, 12288, 4096], P('grp', 'row', 'col')
- posterior: float32 [4096, 4096], P(('grp', 'row'), 'col')
The draws below stay inside these ranges and needn't reach their ends.
Inputs may be any that keep to these rules, and one draw needn't show every extreme that they name: `cover`: the first three slots hold a symmetric positive definite matrix of order 12288 in the column-block order of the steps. `prior`: A symmetric positive definite matrix.
All inputs are finite; a program needn't handle non-finite values.
Results may differ from the reference program's by a relative error of at most 0.0001.
Values sent between devices are 32-bit elements; how exact they have to be, the bound alone decides.
No kernel may reach another device: no remote copies, remote signals or barrier semaphores. Data moves between devices by JAX's collectives and lax.ppermute only.
A program may use at most 192 MiB of HBM per device.

```python
import jax
import jax.numpy as jnp
from jax import lax

M = 12288
CMD = 4096
B = 256
PANELS = 1


def draw_cover(key, part):
    split_keys = jax.random.split(jax.random.fold_in(key, 17), 4)
    inner_rank = max(M // 24, B)
    factors = jax.random.normal(split_keys[0], (M, inner_rank), jnp.float32)
    jitter = jax.random.normal(split_keys[1], (M, M), jnp.float32) * (0.1 / M ** 0.5)
    jitter = (jitter + jitter.T) * 0.7071
    diag_vals = jnp.exp(jax.random.uniform(split_keys[2], (M,), jnp.float32, 0.0, jnp.log(3.0)))
    cross_cov = jnp.clip(jax.random.normal(split_keys[3], (M, CMD), jnp.float32), -6.0, 6.0) * 0.06
    covar = jnp.dot(factors, factors.T, precision=lax.Precision.HIGHEST) / inner_rank + jitter + jnp.diag(diag_vals)
    slots = covar.reshape(M, CMD // B, 3, B).transpose(2, 0, 1, 3).reshape(3, M, CMD)
    return jnp.concatenate([slots, cross_cov[None]], axis=0).astype(jnp.float32)


def draw_prior(key, part):
    split_keys = jax.random.split(jax.random.fold_in(key, 29), 2)
    mixing = jnp.clip(jax.random.normal(split_keys[0], (CMD, CMD), jnp.float32), -6.0, 6.0)
    diag_vals = jnp.exp(jax.random.uniform(split_keys[1], (CMD,), jnp.float32, jnp.log(0.1), jnp.log(0.5)))
    gram = jnp.dot(mixing, mixing.T, precision=lax.Precision.HIGHEST) * (0.2 / CMD)
    gram = (gram + gram.T) * 0.5
    return (gram + jnp.diag(diag_vals)).astype(jnp.float32)


def setup_inputs(seed: int = 0) -> dict:
    arg_keys = jax.random.split(jax.random.key(seed), 3)
    return {
        "cover": draw_cover(jax.random.fold_in(arg_keys[2], 71), 0),
        "prior": draw_prior(jax.random.fold_in(arg_keys[2], 71), 0),
    }


precise = lax.Precision.HIGHEST

def advance(region, row_ids, block_ids, lower_rows, solved, panel):
    update = jnp.dot(lower_rows.astype(jnp.float32), solved.astype(jnp.float32), precision=precise, preferred_element_type=jnp.float32)
    to_right = block_ids > panel
    result = jnp.where((row_ids >= (panel + 1) * B) & to_right, region - update, region)
    own_column = (block_ids[:, :B] == panel) & (row_ids >= panel * B)
    result = jnp.concatenate([jnp.where(own_column, lower_rows, result[:, :B]), result[:, B:]], axis=1)
    stripe = jnp.where(to_right, solved, result[panel * B:(panel + 1) * B])
    return jnp.concatenate([result[:panel * B], stripe, result[(panel + 1) * B:]], axis=0)

def reference(cover, prior):
    slot_count = cover.shape[0]
    row_ids = jnp.arange(M).astype(jnp.int32)[:, None]
    col_blocks = (jnp.arange(CMD) // B).astype(jnp.int32)
    state = [cover[slot] for slot in range(slot_count)]
    posterior = prior
    for panel in range(PANELS):
        panel_col = state[panel][:, :B]
        factor = jnp.linalg.cholesky(panel_col[panel * B:(panel + 1) * B])
        lower_rows = lax.linalg.triangular_solve(factor, panel_col, left_side=False, lower=True, transpose_a=True)
        fresh = []
        commands = None
        for slot in range(slot_count):
            if slot < slot_count - 1:
                block_ids = (3 * col_blocks + slot).astype(jnp.int32)
            else:
                block_ids = jnp.full((CMD,), M, jnp.int32)
            solved = lax.linalg.triangular_solve(factor, state[slot][panel * B:(panel + 1) * B], left_side=True, lower=True)
            fresh.append(advance(state[slot], row_ids, block_ids[None, :], lower_rows, solved, panel))
            commands = solved
        state = fresh
        posterior = posterior - jnp.dot(commands.T.astype(jnp.float32), commands.astype(jnp.float32), precision=precise, preferred_element_type=jnp.float32)
    return (jnp.stack(state), posterior)
```

```python
import functools

import jax
import jax.numpy as jnp
from jax import lax
from jax.experimental import pallas as pl
from jax.experimental.pallas import tpu as pltpu
from jax.sharding import PartitionSpec as P


B = 256
NB = 64
AXES = ("grp", "row", "col")


def dot(a, b, dims=(((1,), (0,)), ((), ()))):
    return lax.dot_general(
        a, b, dims, precision=lax.Precision.HIGHEST, preferred_element_type=jnp.float32
    )


def split(a):
    high = a.astype(jnp.bfloat16)
    return high, (a - high.astype(jnp.float32)).astype(jnp.bfloat16)


def dot3(a, b, dims=(((1,), (0,)), ((), ()))):
    a_high, a_low = split(a)
    b_high, b_low = split(b)
    f = functools.partial(
        lax.dot_general, dimension_numbers=dims, preferred_element_type=jnp.float32
    )
    return f(a_high, b_high) + (f(a_high, b_low) + f(a_low, b_high))


def eliminate(tile):
    sub = lax.broadcasted_iota(jnp.int32, (8, 128), 0)
    count = NB // 8
    x = [tile[8 * v : 8 * v + 8, :] for v in range(count)]
    full = lambda a: jnp.broadcast_to(a, (8, 128))
    for s in range(count):
        bc = {
            v: [full(x[v][:, 8 * s + k : 8 * s + k + 1]) for k in range(8)]
            for v in range(s, count)
        }
        e = [[full(bc[s][k][i : i + 1, :]) for k in range(i + 1)] for i in range(8)]
        r = [full(x[s][i : i + 1, :]) for i in range(8)]
        inv, m = [], {}
        for j in range(8):
            inv.append(1.0 / e[j][j])
            for i in range(j + 1, 8):
                m[i, j] = e[i][j] * inv[j]
            for i in range(j + 1, 8):
                for l in range(j + 1, i + 1):
                    e[i][l] = e[i][l] - m[i, j] * e[l][j]
                r[i] = r[i] - m[i, j] * r[j]
        if s + 1 < count:
            z = [None] * 8
            for i in range(7, -1, -1):
                t = r[i] * inv[i]
                for k in range(7, i, -1):
                    t = t - m[k, i] * z[k]
                z[i] = t
            for v in range(s + 1, count):
                t0 = bc[v][0] * z[0]
                t1 = bc[v][1] * z[1]
                for k in range(2, 8, 2):
                    t0 = t0 + bc[v][k] * z[k]
                    t1 = t1 + bc[v][k + 1] * z[k + 1]
                x[v] = x[v] - (t0 + t1)
        rows, d = r[0], e[0][0]
        for i in range(1, 8):
            rows = jnp.where(sub == i, r[i], rows)
            d = jnp.where(sub == i, e[i][i], d)
        x[s] = rows * lax.rsqrt(d)
    return jnp.concatenate(x, axis=0)


def factor_kernel(d_ref, g_ref, x_ref):
    n = d_ref.shape[0]
    eye = lambda m: (
        lax.broadcasted_iota(jnp.int32, (m, m), 0) == lax.broadcasted_iota(jnp.int32, (m, m), 1)
    ).astype(jnp.float32)
    x_ref[:, :n] = d_ref[...]
    x_ref[:, n:] = eye(n)
    for lo in range(0, n, NB):
        hi = lo + NB
        tile = jnp.concatenate([x_ref[lo:hi, lo:hi], eye(NB)], axis=1)
        inverse = eliminate(tile)[:, NB:]
        u = dot(inverse, x_ref[lo:hi, :])
        x_ref[lo:hi, :] = u
        if hi < n:
            x_ref[hi:, :] = x_ref[hi:, :] - dot(u[:, hi:n], u, (((0,), (0,)), ((), ())))
    g_ref[...] = x_ref[:, n:]


def inverse_factor(d):
    n = d.shape[0]
    return pl.pallas_call(
        factor_kernel,
        out_shape=jax.ShapeDtypeStruct((n, n), jnp.float32),
        scratch_shapes=[pltpu.VMEM((n, 2 * n), jnp.float32)],
        compiler_params=pltpu.CompilerParams(vmem_limit_bytes=8 << 20),
        cost_estimate=pl.CostEstimate(flops=4_000_000_000, bytes_accessed=1 << 20, transcendentals=0),
        name="factor",
    )(d)


def copy_in(pieces, sems):
    made = [pltpu.make_async_copy(s, d, sems.at[i]) for i, (_, s, d) in enumerate(pieces)]
    for (cond, _, _), c in zip(pieces, made):
        pl.when(cond)(c.start)

    def wait():
        for (cond, _, _), c in zip(pieces, made):
            pl.when(cond)(c.wait)

    return wait


def update_kernel(plan, n_p, n_r, a_ref, g_ref, whole_ref, *refs):
    p_refs = refs[:n_p]
    r_refs = refs[n_p : n_p + n_r]
    out_ref, p_buf, r_buf, w_buf, w3_buf, p_sems, r_sems = refs[n_p + n_r :]
    step = pl.program_id(0)
    group, row, col = (lax.axis_index(a) for a in AXES)
    tile = a_ref.shape[0]

    @pl.when(step == 0)
    def _():
        p_plan, r_plan = plan(group, row, col, whole_ref, p_refs, r_refs, p_buf, r_buf)
        wait_r = copy_in(r_plan, r_sems)
        wait_p = copy_in(p_plan, p_sems)
        wait_r()
        w = dot3(g_ref[...], r_buf[...])
        w_buf[...] = w
        high, low = split(w)
        w3_buf[0:B, :] = high
        w3_buf[B : 2 * B, :] = low
        w3_buf[2 * B :, :] = high
        wait_p()

    lower = dot3(p_buf[pl.ds(step * tile, tile), :], g_ref[...], (((1,), (1,)), ((), ())))
    high, low = split(lower)
    parts = jnp.concatenate([high, high, low], axis=1)
    cols = a_ref.shape[1]
    step_cols = min(512, cols)
    for c in range(0, cols, step_cols):
        out_ref[:, c : c + step_cols] = a_ref[:, c : c + step_cols] - jnp.dot(
            parts, w3_buf[:, c : c + step_cols], preferred_element_type=jnp.float32
        )

    @pl.when((row == 0) & (step * tile < B))
    def _():
        out_ref[0:B, :] = w_buf[...]

    @pl.when((group == 0) & (col == 0))
    def _():
        out_ref[:, 0:B] = lower


def update(plan, sizes, a, g, p_list, r_list):
    rows, cols = a.shape
    tile = 2 * B if rows % (2 * B) == 0 else B
    any_spec = pl.BlockSpec(memory_space=pl.ANY)
    n_p, n_r = len(p_list), len(r_list)
    n_pp, n_rp = sizes
    return pl.pallas_call(
        functools.partial(update_kernel, plan, n_p, n_r),
        grid=(rows // tile,),
        in_specs=[
            pl.BlockSpec((tile, cols), lambda i: (i, 0)),
            pl.BlockSpec((B, B), lambda i: (0, 0)),
            any_spec,
        ]
        + [any_spec] * (n_p + n_r),
        out_specs=pl.BlockSpec((tile, cols), lambda i: (i, 0)),
        out_shape=jax.ShapeDtypeStruct((rows, cols), jnp.float32),
        scratch_shapes=[
            pltpu.VMEM((rows, B), jnp.float32),
            pltpu.VMEM((B, cols), jnp.float32),
            pltpu.VMEM((B, cols), jnp.float32),
            pltpu.VMEM((3 * B, cols), jnp.bfloat16),
            pltpu.SemaphoreType.DMA((n_pp,)),
            pltpu.SemaphoreType.DMA((n_rp,)),
        ],
        compiler_params=pltpu.CompilerParams(vmem_limit_bytes=62 << 20),
        cost_estimate=pl.CostEstimate(
            flops=6 * rows * cols * B, bytes_accessed=8 * rows * cols, transcendentals=0
        ),
        name="update",
    )(a, g, a, *p_list, *r_list)


def posterior_kernel(prior_ref, g_ref, win_ref, x_ref, out_ref):
    g = g_ref[...]
    y = dot3(g, x_ref[...])
    y_win = dot3(g, win_ref[...])
    out_ref[...] = prior_ref[...] - dot3(y_win, y, (((0,), (0,)), ((), ())))


def posterior_update(prior, g, window, x):
    return pl.pallas_call(
        posterior_kernel,
        out_shape=jax.ShapeDtypeStruct(prior.shape, jnp.float32),
        compiler_params=pltpu.CompilerParams(vmem_limit_bytes=32 << 20),
        cost_estimate=pl.CostEstimate(
            flops=6 * prior.shape[0] * prior.shape[1] * B,
            bytes_accessed=6 * prior.size,
            transcendentals=0,
        ),
        name="posterior",
    )(prior, g, window, x)


def panel(cover, prior):
    a = cover[0]
    group, row, col = (lax.axis_index(x) for x in AXES)
    gn, rn, cn = (lax.axis_size(x) for x in AXES)
    rows, cols = a.shape
    core = group % 2
    ident = lambda g, r, c: (g * rn + r) * cn + c

    def send(x, pairs):
        return lax.ppermute(x, AXES, [(ident(*s), ident(*d)) for s, d in pairs])

    all_r, all_c = range(rn), range(cn)
    mid = rn // 2
    others = [r for r in range(1, rn) if r != mid]

    steps = []
    d = 1
    while d < cn:
        steps.append(d)
        d *= 2
    along_x = [((0, c), (x, c)) for c in all_c for x in range(1, gn // 2)]

    def tree(c_first):
        out = []
        for d in steps:
            xs = [0] if c_first else range(gn // 2)
            out.append([((x, c), (x, c + d)) for x in xs for c in range(d)])
        if c_first:
            return out + [along_x]
        return [[p for p in along_x if p[0][1] == 0]] + out

    def on_cores(first, second):
        return [
            ((2 * x + k, r, c), (2 * x_ + k, r, c_))
            for k, pairs in ((0, first), (1, second))
            for (x, c), (x_, c_) in pairs
            for r in all_r
        ]

    diag = jnp.where((group == 0) & (row == 0) & (col == 0), a[0:B, 0:B], 0.0)
    diag = diag + sum(send(diag, [((0, 0, 0), (0, r, 0))]) for r in range(1, rn))
    diag = diag + send(diag, [((0, r, 0), (1, r, 0)) for r in all_r])
    if (gn, cn) == (4, 2):
        hops = [
            [((0, 0), (0, 1)), ((1, 0), (3, 0))],
            [((3, 0), (2, 0)), ((0, 1), (2, 1))],
            [((0, 1), (1, 1)), ((2, 1), (3, 1))],
        ]
        hops = [[((p, r, c), (q, r, e)) for (p, c), (q, e) in h for r in all_r] for h in hops]
    else:
        hops = [on_cores(*pair) for pair in zip(tree(True), tree(False))]
    for pairs in hops:
        diag = diag + send(diag, pairs)
    g = inverse_factor(diag)

    half = rows // 2
    top, bottom = a[:half, 0:B], a[half:, 0:B]
    firsts, seconds = tree(False), tree(True)
    source = lambda p: p[0] == (0, 0)
    part = send(bottom, [((0, r, 0), (1, r, 0)) for r in all_r])
    part = part + send(top, on_cores(filter(source, firsts[0]), []))
    part = part + send(
        bottom, [((0, r, 0), (2 * x + 1, r, c)) for _, (x, c) in seconds[0] for r in all_r]
    )
    part = jnp.where((group == 0) & (col == 0), top, part)
    for pair in zip(firsts[1:], seconds[1:]):
        part = part + send(part, on_cores(*pair))
    rest = send(part, [((g_, r, c), (g_ ^ 1, r, c)) for g_ in range(gn) for r in all_r for c in all_c])

    last = gn - 1
    units = cols // 128
    u = -(-units * 5 // 16)
    widths = [128 * u, 128 * max(1, units * 3 // 8)]
    widths.append(cols - sum(widths))
    starts = [0, widths[0], widths[0] + widths[1]]
    each = [(g_, c) for g_ in range(gn) for c in all_c]
    r_list, r_keys, xs = [], [], []
    own = lax.optimization_barrier([a[0:B, s : s + w] for s, w in zip(starts, widths)])
    mids = [send(p, [((g_, 0, c), (g_, mid, c)) for g_, c in each]) for p in own]
    for s, w, p, m in zip(starts, widths, own, mids):
        r_list.append(m)
        r_keys.append((s, w, mid))
        got = m
        for r in others:
            o = send(m, [((g_, mid, c), (g_, r, c)) for g_, c in each])
            r_list.append(o)
            r_keys.append((s, w, r))
            got = got + o
        got = jnp.where(group == last, jnp.where(row == 0, p, got), 0.0)
        for to in range(1, last, 2):
            got = got + send(got, [((last, r, c), (to, r, c)) for r in all_r for c in all_c])
        xs.append(got)

    def plan(group, row, col, whole, p_refs, r_refs, p_buf, r_buf):
        even = lax.rem(group, 2) == 0
        top, bottom = p_buf.at[:half, :], p_buf.at[half:, :]
        p_plan = [
            (even, p_refs[0], top),
            (even, p_refs[1], bottom),
            (~even, p_refs[1], top),
            (~even, p_refs[0], bottom),
        ]
        r_plan = [(row == 0, whole.at[0:B, :], r_buf)]
        for (s, w, r), ref in zip(r_keys, r_refs):
            r_plan.append((row == r, ref, r_buf.at[:, s : s + w]))
        return p_plan, r_plan

    block = update(plan, (4, 1 + len(r_keys)), a, g, [part, rest], r_list)

    width = prior.shape[0]
    x = jnp.concatenate(xs, axis=1)
    down = [((g_, r, c), (g_ - 1, r, c)) for g_ in range(1, gn, 2) for r in all_r for c in all_c]
    x_over = send(x, down)
    owner = lambda g_, r: (g_ * rn + r) * width // cols

    def window_of(shift):
        first = ((group - shift) * rn + row) * width
        piece = lax.dynamic_slice_in_dim(x, lax.rem(first + gn * cols, cols), width, 1)
        got = [
            send(
                piece,
                [
                    ((g_, r, owner(g_ - shift, r)), (g_, r, (owner(g_ - shift, r) + d) % cn))
                    for g_ in range(1, gn, 2)
                    for r in all_r
                ],
            )
            for d in range(1, cn)
        ]
        return jnp.where(first // cols == col, piece, sum(got))

    window = window_of(0)
    window_over = send(window_of(1), down)
    window = jnp.where(core == 1, window, window_over)
    x = jnp.where(core == 1, x, x_over)
    return block[None], posterior_update(prior, g, window, x)


def solution(mesh):
    return jax.shard_map(
        panel,
        mesh=mesh,
        in_specs=(P("grp", "row", "col"), P(("grp", "row"), "col")),
        out_specs=(P("grp", "row", "col"), P(("grp", "row"), "col")),
        check_vma=False,
    )
```

```python
import functools

import jax
import jax.numpy as jnp
from jax import lax
from jax.experimental import pallas as pl
from jax.experimental.pallas import tpu as pltpu
from jax.sharding import PartitionSpec as P


B = 256
NB = 64
AXES = ("grp", "row", "col")


def dot(a, b, dims=(((1,), (0,)), ((), ()))):
    return lax.dot_general(
        a, b, dims, precision=lax.Precision.HIGHEST, preferred_element_type=jnp.float32
    )


def split(a):
    high = a.astype(jnp.bfloat16)
    return high, (a - high.astype(jnp.float32)).astype(jnp.bfloat16)


def dot3(a, b, dims=(((1,), (0,)), ((), ()))):
    a_high, a_low = split(a)
    b_high, b_low = split(b)
    f = functools.partial(
        lax.dot_general, dimension_numbers=dims, preferred_element_type=jnp.float32
    )
    return f(a_high, b_high) + (f(a_high, b_low) + f(a_low, b_high))


def eliminate(tile):
    sub = lax.broadcasted_iota(jnp.int32, (8, 128), 0)
    count = NB // 8
    x = [tile[8 * v : 8 * v + 8, :] for v in range(count)]
    full = lambda a: jnp.broadcast_to(a, (8, 128))
    for s in range(count):
        bc = {
            v: [full(x[v][:, 8 * s + k : 8 * s + k + 1]) for k in range(8)]
            for v in range(s, count)
        }
        e = [[full(bc[s][k][i : i + 1, :]) for k in range(i + 1)] for i in range(8)]
        r = [full(x[s][i : i + 1, :]) for i in range(8)]
        inv, m = [], {}
        for j in range(8):
            inv.append(1.0 / e[j][j])
            for i in range(j + 1, 8):
                m[i, j] = e[i][j] * inv[j]
            for i in range(j + 1, 8):
                for l in range(j + 1, i + 1):
                    e[i][l] = e[i][l] - m[i, j] * e[l][j]
                r[i] = r[i] - m[i, j] * r[j]
        if s + 1 < count:
            z = [None] * 8
            for i in range(7, -1, -1):
                t = r[i] * inv[i]
                for k in range(7, i, -1):
                    t = t - m[k, i] * z[k]
                z[i] = t
            for v in range(s + 1, count):
                t0 = bc[v][0] * z[0]
                t1 = bc[v][1] * z[1]
                for k in range(2, 8, 2):
                    t0 = t0 + bc[v][k] * z[k]
                    t1 = t1 + bc[v][k + 1] * z[k + 1]
                x[v] = x[v] - (t0 + t1)
        rows, d = r[0], e[0][0]
        for i in range(1, 8):
            rows = jnp.where(sub == i, r[i], rows)
            d = jnp.where(sub == i, e[i][i], d)
        x[s] = rows * lax.rsqrt(d)
    return jnp.concatenate(x, axis=0)


def factor_kernel(d_ref, g_ref, x_ref):
    n = d_ref.shape[0]
    eye = lambda m: (
        lax.broadcasted_iota(jnp.int32, (m, m), 0) == lax.broadcasted_iota(jnp.int32, (m, m), 1)
    ).astype(jnp.float32)
    x_ref[:, :n] = d_ref[...]
    x_ref[:, n:] = eye(n)
    for lo in range(0, n, NB):
        hi = lo + NB
        tile = jnp.concatenate([x_ref[lo:hi, lo:hi], eye(NB)], axis=1)
        inverse = eliminate(tile)[:, NB:]
        u = dot(inverse, x_ref[lo:hi, :])
        x_ref[lo:hi, :] = u
        if hi < n:
            x_ref[hi:, :] = x_ref[hi:, :] - dot(u[:, hi:n], u, (((0,), (0,)), ((), ())))
    g_ref[...] = x_ref[:, n:]


def inverse_factor(d):
    n = d.shape[0]
    return pl.pallas_call(
        factor_kernel,
        out_shape=jax.ShapeDtypeStruct((n, n), jnp.float32),
        scratch_shapes=[pltpu.VMEM((n, 2 * n), jnp.float32)],
        compiler_params=pltpu.CompilerParams(vmem_limit_bytes=8 << 20),
        cost_estimate=pl.CostEstimate(flops=4_000_000_000, bytes_accessed=1 << 20, transcendentals=0),
        name="factor",
    )(d)


def copy_in(pieces, sems):
    made = [pltpu.make_async_copy(s, d, sems.at[i]) for i, (_, s, d) in enumerate(pieces)]
    for (cond, _, _), c in zip(pieces, made):
        pl.when(cond)(c.start)

    def wait():
        for (cond, _, _), c in zip(pieces, made):
            pl.when(cond)(c.wait)

    return wait


def subtract_product(a_ref, g_ref, p_buf, w3_ref, out_ref):
    step = pl.program_id(0)
    tile, cols = a_ref.shape
    lower = dot3(p_buf[pl.ds(step * tile, tile), :], g_ref[...], (((1,), (1,)), ((), ())))
    high, low = split(lower)
    parts = jnp.concatenate([high, high, low], axis=1)
    width = min(512, cols)
    for c in range(0, cols, width):
        out_ref[:, c : c + width] = a_ref[:, c : c + width] - jnp.dot(
            parts, w3_ref[:, c : c + width], preferred_element_type=jnp.float32
        )
    return lower


def top_kernel(plan, n_r, a_ref, g_ref, whole_ref, part_ref, rest_ref, *refs):
    r_refs = refs[:n_r]
    out_ref, w3_ref, p_buf, r_buf, w_buf, p_sems, r_sems = refs[n_r:]
    step = pl.program_id(0)
    group, row, col = (lax.axis_index(a) for a in AXES)
    even = lax.rem(group, 2) == 0

    @pl.when(step == 0)
    def _():
        wait_r = copy_in(plan(row, whole_ref, r_refs, r_buf), r_sems)
        wait_p = copy_in([(even, part_ref, p_buf), (~even, rest_ref, p_buf)], p_sems)
        wait_r()
        w = dot3(g_ref[...], r_buf[...])
        w_buf[...] = w
        high, low = split(w)
        w3_ref[0:B, :] = high
        w3_ref[B : 2 * B, :] = low
        w3_ref[2 * B :, :] = high
        wait_p()

    lower = subtract_product(a_ref, g_ref, p_buf, w3_ref, out_ref)

    @pl.when((row == 0) & (step == 0))
    def _():
        out_ref[0:B, :] = w_buf[...]

    @pl.when((group == 0) & (col == 0))
    def _():
        out_ref[:, 0:B] = lower


def bottom_kernel(a_ref, g_ref, w3_ref, part_ref, rest_ref, prev_ref, out_ref, p_buf, p_sems):
    group, col = lax.axis_index(AXES[0]), lax.axis_index(AXES[2])
    even = lax.rem(group, 2) == 0

    @pl.when(pl.program_id(0) == 0)
    def _():
        copy_in([(even, rest_ref, p_buf), (~even, part_ref, p_buf)], p_sems)()

    lower = subtract_product(a_ref, g_ref, p_buf, w3_ref, out_ref)

    @pl.when((group == 0) & (col == 0))
    def _():
        out_ref[:, 0:B] = lower


def update_specs(a):
    rows, cols = a.shape
    half = rows // 2
    tile = 2 * B if half % (2 * B) == 0 else B
    params = dict(
        grid=(half // tile,),
        compiler_params=pltpu.CompilerParams(vmem_limit_bytes=62 << 20),
        cost_estimate=pl.CostEstimate(
            flops=3 * rows * cols * B, bytes_accessed=4 * rows * cols, transcendentals=0
        ),
    )
    fixed = lambda shape: pl.BlockSpec(shape, lambda i: (0, 0))
    rows_from = lambda first: pl.BlockSpec((tile, cols), lambda i: (i + first // tile, 0))
    return half, params, fixed, rows_from, pl.BlockSpec(memory_space=pl.ANY)


def update_top(plan, n_copies, a, g, part, rest, r_list):
    rows, cols = a.shape
    half, params, fixed, rows_from, anywhere = update_specs(a)
    return pl.pallas_call(
        functools.partial(top_kernel, plan, len(r_list)),
        in_specs=[rows_from(0), fixed((B, B))] + [anywhere] * (3 + len(r_list)),
        out_specs=[rows_from(0), fixed((3 * B, cols))],
        out_shape=[
            jax.ShapeDtypeStruct((rows, cols), jnp.float32),
            jax.ShapeDtypeStruct((3 * B, cols), jnp.bfloat16),
        ],
        scratch_shapes=[
            pltpu.VMEM((half, B), jnp.float32),
            pltpu.VMEM((B, cols), jnp.float32),
            pltpu.VMEM((B, cols), jnp.float32),
            pltpu.SemaphoreType.DMA((2,)),
            pltpu.SemaphoreType.DMA((n_copies,)),
        ],
        name="top",
        **params,
    )(a, g, a, part, rest, *r_list)


def update_bottom(a, g, w3, part, rest, prev):
    rows, cols = a.shape
    half, params, fixed, rows_from, anywhere = update_specs(a)
    return pl.pallas_call(
        bottom_kernel,
        in_specs=[rows_from(half), fixed((B, B)), fixed((3 * B, cols))] + [anywhere] * 3,
        out_specs=rows_from(half),
        out_shape=jax.ShapeDtypeStruct((rows, cols), jnp.float32),
        input_output_aliases={5: 0},
        scratch_shapes=[pltpu.VMEM((half, B), jnp.float32), pltpu.SemaphoreType.DMA((2,))],
        name="bottom",
        **params,
    )(a, g, w3, part, rest, prev)


def posterior_kernel(prior_ref, g_ref, win_ref, x_ref, out_ref):
    g = g_ref[...]
    y = dot3(g, x_ref[...])
    y_win = dot3(g, win_ref[...])
    out_ref[...] = prior_ref[...] - dot3(y_win, y, (((0,), (0,)), ((), ())))


def posterior_update(prior, g, window, x):
    return pl.pallas_call(
        posterior_kernel,
        out_shape=jax.ShapeDtypeStruct(prior.shape, jnp.float32),
        compiler_params=pltpu.CompilerParams(vmem_limit_bytes=32 << 20),
        cost_estimate=pl.CostEstimate(
            flops=6 * prior.shape[0] * prior.shape[1] * B,
            bytes_accessed=6 * prior.size,
            transcendentals=0,
        ),
        name="posterior",
    )(prior, g, window, x)


def panel(cover, prior):
    a = cover[0]
    group, row, col = (lax.axis_index(x) for x in AXES)
    gn, rn, cn = (lax.axis_size(x) for x in AXES)
    rows, cols = a.shape
    core = group % 2
    ident = lambda g, r, c: (g * rn + r) * cn + c

    def send(x, pairs):
        return lax.ppermute(x, AXES, [(ident(*s), ident(*d)) for s, d in pairs])

    all_r, all_c = range(rn), range(cn)
    mid = rn // 2
    others = [r for r in range(1, rn) if r != mid]

    steps = []
    d = 1
    while d < cn:
        steps.append(d)
        d *= 2
    along_x = [((0, c), (x, c)) for c in all_c for x in range(1, gn // 2)]

    def tree(c_first):
        out = []
        for d in steps:
            xs = [0] if c_first else range(gn // 2)
            out.append([((x, c), (x, c + d)) for x in xs for c in range(d)])
        if c_first:
            return out + [along_x]
        return [[p for p in along_x if p[0][1] == 0]] + out

    def on_cores(first, second):
        return [
            ((2 * x + k, r, c), (2 * x_ + k, r, c_))
            for k, pairs in ((0, first), (1, second))
            for (x, c), (x_, c_) in pairs
            for r in all_r
        ]

    diag = jnp.where((group == 0) & (row == 0) & (col == 0), a[0:B, 0:B], 0.0)
    diag = diag + sum(send(diag, [((0, 0, 0), (0, r, 0))]) for r in range(1, rn))
    diag = diag + send(diag, [((0, r, 0), (1, r, 0)) for r in all_r])
    if (gn, cn) == (4, 2):
        hops = [
            [((0, 0), (0, 1)), ((1, 0), (3, 0))],
            [((3, 0), (2, 0)), ((0, 1), (2, 1))],
            [((0, 1), (1, 1)), ((2, 1), (3, 1))],
        ]
        hops = [[((p, r, c), (q, r, e)) for (p, c), (q, e) in h for r in all_r] for h in hops]
    else:
        hops = [on_cores(*pair) for pair in zip(tree(True), tree(False))]
    for pairs in hops:
        diag = diag + send(diag, pairs)
    g = inverse_factor(diag)

    half = rows // 2
    top, bottom = a[:half, 0:B], a[half:, 0:B]
    firsts, seconds = tree(False), tree(True)
    source = lambda p: p[0] == (0, 0)
    part = send(bottom, [((0, r, 0), (1, r, 0)) for r in all_r])
    part = part + send(top, on_cores(filter(source, firsts[0]), []))
    part = part + send(
        bottom, [((0, r, 0), (2 * x + 1, r, c)) for _, (x, c) in seconds[0] for r in all_r]
    )
    part = jnp.where((group == 0) & (col == 0), top, part)
    for pair in zip(firsts[1:], seconds[1:]):
        part = part + send(part, on_cores(*pair))
    rest = send(part, [((g_, r, c), (g_ ^ 1, r, c)) for g_ in range(gn) for r in all_r for c in all_c])

    last = gn - 1
    units = cols // 128
    u = -(-units * 5 // 16)
    widths = [128 * u, 128 * max(1, units * 3 // 8)]
    widths.append(cols - sum(widths))
    starts = [0, widths[0], widths[0] + widths[1]]
    each = [(g_, c) for g_ in range(gn) for c in all_c]
    r_list, r_keys, xs = [], [], []
    own = lax.optimization_barrier([a[0:B, s : s + w] for s, w in zip(starts, widths)])
    mids = [send(p, [((g_, 0, c), (g_, mid, c)) for g_, c in each]) for p in own]
    for s, w, p, m in zip(starts, widths, own, mids):
        r_list.append(m)
        r_keys.append((s, w, mid))
        got = m
        for r in others:
            o = send(m, [((g_, mid, c), (g_, r, c)) for g_, c in each])
            r_list.append(o)
            r_keys.append((s, w, r))
            got = got + o
        got = jnp.where(group == last, jnp.where(row == 0, p, got), 0.0)
        for to in range(1, last, 2):
            got = got + send(got, [((last, r, c), (to, r, c)) for r in all_r for c in all_c])
        xs.append(got)

    def plan(row, whole, r_refs, r_buf):
        out = [(row == 0, whole.at[0:B, :], r_buf)]
        for (s, w, r), ref in zip(r_keys, r_refs):
            out.append((row == r, ref, r_buf.at[:, s : s + w]))
        return out

    block, w3 = update_top(plan, 1 + len(r_keys), a, g, part, rest, r_list)
    block = update_bottom(a, g, w3, part, rest, block)

    width = prior.shape[0]
    x = jnp.concatenate(xs, axis=1)
    down = [((g_, r, c), (g_ - 1, r, c)) for g_ in range(1, gn, 2) for r in all_r for c in all_c]
    x_over = send(x, down)
    owner = lambda g_, r: (g_ * rn + r) * width // cols

    def window_of(shift):
        first = ((group - shift) * rn + row) * width
        piece = lax.dynamic_slice_in_dim(x, lax.rem(first + gn * cols, cols), width, 1)
        got = [
            send(
                piece,
                [
                    ((g_, r, owner(g_ - shift, r)), (g_, r, (owner(g_ - shift, r) + d) % cn))
                    for g_ in range(1, gn, 2)
                    for r in all_r
                ],
            )
            for d in range(1, cn)
        ]
        return jnp.where(first // cols == col, piece, sum(got))

    window = window_of(0)
    window_over = send(window_of(1), down)
    window = jnp.where(core == 1, window, window_over)
    x = jnp.where(core == 1, x, x_over)
    return block[None], posterior_update(prior, g, window, x)


def solution(mesh):
    return jax.shard_map(
        panel,
        mesh=mesh,
        in_specs=(P("grp", "row", "col"), P(("grp", "row"), "col")),
        out_specs=(P("grp", "row", "col"), P(("grp", "row"), "col")),
        check_vma=False,
    )
```
